256 devices in a mesh: groups: 2 (over y), seq: 16 (over z), section: 4 (over x), mp: 2 (over core).
Axes of the slice: x: 4, y: 2, z: 16, core: 2. Of those that a mesh axis runs over, the one named last changes fastest.
The devices are a block of a 4x16x16 slice.
Arguments:
- light_queries: bfloat16 [8192, 8192], P(('groups', 'seq'), ('section', 'mp')), parts along dimension 0, may hold values from -6 to 6
- light_keys: bfloat16 [8192, 8192], P(('groups', 'seq'), ('section', 'mp')), parts along dimension 0, may hold values from -6 to 6
- light_values: bfloat16 [8192, 8192], P(('groups', 'seq'), ('section', 'mp')), parts along dimension 0, may hold values from -6 to 6
- decay_log: float32 [8192, 64], P(('groups', 'seq'), ('section', 'mp')), parts along dimension 0, may hold values from -1 to 0
- norm_gain: float32 [8192], P(('section', 'mp')), may hold values from 0.25 to 1.75
- soft_queries: bfloat16 [8192, 8192], P(('groups', 'seq'), ('section', 'mp')), parts along dimension 0, may hold values from -150 to 150
- soft_keys: bfloat16 [8192, 1024], P(('groups', 'seq'), ('section', 'mp')), parts along dimension 0, may hold values from -6 to 6
- soft_values: bfloat16 [8192, 1024], P(('groups', 'seq'), ('section', 'mp')), parts along dimension 0, may hold values from -6 to 6
- lengths: int32 [32], P('groups'), parts along dimension 0, may hold values from 1 to 256, 3072 in all
Outputs:
- light_out: bfloat16 [8192, 8192], P(('groups', 'seq'), ('section', 'mp')), parts along dimension 0
- soft_out: bfloat16 [8192, 8192], P(('groups', 'seq'), ('section', 'mp')), parts along dimension 0
The draws below stay inside these ranges and needn't reach their ends.
There are 2 independent parts, one for each index of `groups`. The reference program is written for one: setup_inputs(seed, part) draws one part's arguments, and reference() takes and returns one part's arrays. A program takes and returns all parts, laid end to end along the dimension named above; an argument that names none is the same for every part. Nothing has to cross between parts.
Inputs may be any that keep to these rules, and one draw needn't show every extreme that they name: The live tokens of a block stand at its first slots; the lengths sum to 3072.
All inputs are finite; a program needn't handle non-finite values.
Results may differ from the reference program's by a relative error of at most 0.007.
Values may be sent and summed in bfloat16 or wider, within the bound.
A program may use at most 64 MiB of HBM per device.

```python
import math
import jax
import jax.numpy as jnp
import numpy as np
from jax import lax

QUERY_HEAD_COUNT = 64
KV_HEADS = 8
HEAD_DIM = 128
TOK_DEV = 256
TOKEN_SLOTS = 4096
N_SEQ = 16


def draw_decay_log(key, part):
    random_subkeys = jax.random.split(jax.random.fold_in(key, 3), 8)
    slow_share = 0.5
    slow_heads = jax.random.uniform(random_subkeys[0], (QUERY_HEAD_COUNT,)) < slow_share
    slow_rate = jax.random.uniform(random_subkeys[1], (QUERY_HEAD_COUNT,), minval=0.05, maxval=0.2) * math.log(10.0) / TOKEN_SLOTS
    fast_rate = 1.0 / jax.random.uniform(random_subkeys[2], (QUERY_HEAD_COUNT,), minval=30.0, maxval=50.0)
    head_decay_rate = jnp.where(slow_heads, slow_rate, fast_rate)
    block_count = TOKEN_SLOTS // TOK_DEV
    block_multiplier = jnp.repeat(jax.random.uniform(random_subkeys[3], (block_count, QUERY_HEAD_COUNT), minval=0.6, maxval=1.4), TOK_DEV, axis=0)
    slot_multiplier = jax.random.uniform(random_subkeys[4], (TOKEN_SLOTS, QUERY_HEAD_COUNT), minval=0.5, maxval=1.5)
    first_position = jax.random.randint(random_subkeys[5], (QUERY_HEAD_COUNT,), 0, TOKEN_SLOTS)
    position_gap = jax.random.randint(random_subkeys[7], (QUERY_HEAD_COUNT,), 1, TOKEN_SLOTS)
    second_position = (first_position + position_gap) % TOKEN_SLOTS
    group_length = jax.random.uniform(random_subkeys[6], (2, QUERY_HEAD_COUNT), minval=math.log(0.5), maxval=math.log(0.8))
    token_slot_index = jnp.arange(TOKEN_SLOTS)[:, None]
    token_groups = jnp.where(token_slot_index == first_position[None, :], group_length[0][None, :], 0.0)
    token_groups = token_groups + jnp.where(token_slot_index == second_position[None, :], group_length[1][None, :], 0.0)
    return (-head_decay_rate[None, :] * block_multiplier * slot_multiplier + token_groups).astype(jnp.float32)


def soft_pair(key):
    first_key, second_key = jax.random.split(jax.random.fold_in(key, 17))
    queries = jnp.clip(jax.random.normal(first_key, (TOKEN_SLOTS, QUERY_HEAD_COUNT * HEAD_DIM), jnp.float32), -6.0, 6.0)
    keys_drawn = jnp.clip(jax.random.normal(second_key, (TOKEN_SLOTS, KV_HEADS * HEAD_DIM), jnp.float32), -6.0, 6.0)
    return (queries, keys_drawn)


def draw_soft_queries(key, part):
    return soft_pair(key)[0].astype(jnp.bfloat16)


def draw_soft_keys(key, part):
    return soft_pair(key)[1].astype(jnp.bfloat16)


def block_levels(own_key, extent, cuts, least, largest):
    level, own = 1.0, jax.random.fold_in(own_key, 6)
    for dim, blocks in cuts:
        heights = jnp.exp(jax.random.uniform(jax.random.fold_in(own, dim), (blocks,), jnp.float32, least / len(cuts), largest / len(cuts)))
        level = level * jnp.repeat(heights, extent[dim] // blocks).reshape([-1 if axis == dim else 1 for axis in range(len(extent))])
    return level


def profile(amount, total, reach, lean):
    loads = [(1 << 20) // math.isqrt(rank ** lean) + 1 for rank in range(2, amount + 1)]
    rest, given = total - reach - (amount - 1), [1] * (amount - 1)
    while rest > 0:
        movable = [i for i in range(amount - 1) if given[i] < reach]
        mass, remaining = sum([loads[i] for i in movable]), rest
        for i in movable:
            more = min(reach - given[i], max(1, remaining * loads[i] // mass), rest)
            given[i] = given[i] + more
            rest = rest - more
    return np.array([reach] + given)


def uneven(own_key, amount, total, bound, slope):
    if amount == 2:
        one = jax.random.randint(own_key, (), max(1, total - bound), min(bound, total - 1) + 1)
        return jnp.stack([one, total - one])
    tallies = jnp.asarray(profile(amount, total, bound, slope), jnp.int32)
    couples = (amount - 1) // 2
    source_of, receiver = tallies[1:1 + 2 * couples:2], tallies[2:2 + 2 * couples:2]
    slack = jnp.minimum(source_of - 1, bound - receiver)
    passed = jax.random.randint(jax.random.fold_in(own_key, 1), (couples,), 0, 1 << 20) % (slack + 1)
    tallies = tallies.at[1:1 + 2 * couples:2].set(source_of - passed).at[2:2 + 2 * couples:2].set(receiver + passed)
    return tallies[jax.random.permutation(jax.random.fold_in(own_key, 2), amount)]


def centred(key, shape, spread, limit, pieces=(), held_as=jnp.bfloat16):
    array = jax.random.normal(key, shape, jnp.float32) * spread
    if len(pieces) > 0:
        array = block_levels(key, shape, pieces, -0.22, 0.18) * array
    return jnp.clip(array, min=-limit, max=limit).astype(held_as)


def setup_inputs(seed: int = 0, part: int = 0) -> dict:
    streams_of = jax.random.split(jax.random.key(seed), 10)
    own_keys = jax.random.split(jax.random.fold_in(streams_of[9], part), 10)
    return {
        "light_queries": centred(own_keys[0], (TOKEN_SLOTS, QUERY_HEAD_COUNT * HEAD_DIM), 1.0, 6.0, ((0, 16), (1, 8))),
        "light_keys": centred(own_keys[1], (TOKEN_SLOTS, QUERY_HEAD_COUNT * HEAD_DIM), 1.0, 6.0, ((0, 16), (1, 8))),
        "light_values": centred(own_keys[2], (TOKEN_SLOTS, QUERY_HEAD_COUNT * HEAD_DIM), 1.0, 6.0, ((0, 16), (1, 8))),
        "decay_log": draw_decay_log(jax.random.fold_in(jax.random.fold_in(streams_of[9], part), 71), part),
        "norm_gain": jnp.clip(1.0 + 0.15 * jax.random.normal(streams_of[4], (QUERY_HEAD_COUNT * HEAD_DIM,), jnp.float32), 0.25, 1.75),
        "soft_queries": draw_soft_queries(jax.random.fold_in(jax.random.fold_in(streams_of[9], part), 71), part),
        "soft_keys": draw_soft_keys(jax.random.fold_in(jax.random.fold_in(streams_of[9], part), 71), part),
        "soft_values": centred(own_keys[7], (TOKEN_SLOTS, KV_HEADS * HEAD_DIM), 1.0, 6.0, ((0, 16), (1, 8))),
        "lengths": uneven(own_keys[8], N_SEQ, TOKEN_SLOTS * 3 // 4, TOK_DEV, 2).astype(jnp.int32),
    }


EPSILON = 1e-06

def rounded(values):
    return lax.optimization_barrier(values.astype(jnp.bfloat16)).astype(jnp.float32)

def light_reference(light_queries, light_keys, light_values, decay_log, norm_gain, lengths):
    block_shape = (N_SEQ, TOK_DEV, QUERY_HEAD_COUNT, HEAD_DIM)
    queries = light_queries.reshape(block_shape).astype(jnp.float32)
    keys_all = light_keys.reshape(block_shape).astype(jnp.float32)
    values_all = light_values.reshape(block_shape).astype(jnp.float32)
    decays = decay_log.reshape(N_SEQ, TOK_DEV, QUERY_HEAD_COUNT)
    score_scale = HEAD_DIM ** (-0.5)
    token_slot_index = jnp.arange(TOK_DEV, dtype=jnp.int32)
    causal = token_slot_index[:, None] >= token_slot_index[None, :]
    gain_heads = norm_gain.reshape(QUERY_HEAD_COUNT, HEAD_DIM)

    def advance(entering, inputs):
        query_block, key_block, value_block, decay_block, length = inputs
        live_rows = token_slot_index < length
        masked = jnp.where(live_rows[:, None], decay_block, 0.0)
        running = jnp.cumsum(masked, axis=0)
        ending = running[-1]
        scores = jnp.einsum('thd,shd->hts', query_block, key_block)
        log_gaps = running.T[:, :, None] - running.T[:, None, :]
        allowed = causal[None] & live_rows[None, None, :]
        weights = jnp.where(allowed, jnp.exp(jnp.where(causal[None], log_gaps, 0.0)), 0.0)
        intra_weight = rounded(scores * score_scale * weights)
        inside = jnp.einsum('hts,shd->thd', intra_weight, value_block)
        across = jnp.einsum('thd,hde->the', query_block * score_scale, entering, precision=lax.Precision.HIGHEST) * jnp.exp(running)[:, :, None]
        combined = inside + across
        normed = combined * lax.rsqrt(lax.optimization_barrier(jnp.mean(combined * combined, axis=-1, keepdims=True)) + EPSILON) * gain_heads
        output = jnp.where(live_rows[:, None, None], normed, 0.0)
        fading = jnp.exp(ending[None, :] - running) * live_rows[:, None]
        block_keys = rounded(key_block * fading[:, :, None])
        block_state = jnp.einsum('thd,the->hde', block_keys, value_block)
        leaving = jnp.exp(ending)[:, None, None] * entering + block_state
        return (leaving, output)
    initial = jnp.zeros((QUERY_HEAD_COUNT, HEAD_DIM, HEAD_DIM), jnp.float32)
    final_state, outputs = lax.scan(advance, initial, (queries, keys_all, values_all, decays, lengths))
    return outputs.astype(jnp.bfloat16).reshape(TOKEN_SLOTS, QUERY_HEAD_COUNT * HEAD_DIM)

def soft_reference(soft_queries, soft_keys, soft_values, live_all):
    group_size = QUERY_HEAD_COUNT // KV_HEADS
    score_scale = HEAD_DIM ** (-0.5)
    queries = soft_queries.reshape(N_SEQ, TOK_DEV, KV_HEADS, group_size, HEAD_DIM)
    keys_all = soft_keys.reshape(TOKEN_SLOTS, KV_HEADS, HEAD_DIM).transpose(1, 0, 2)
    values_all = soft_values.reshape(TOKEN_SLOTS, KV_HEADS, HEAD_DIM).transpose(1, 0, 2)
    positions = jnp.arange(TOKEN_SLOTS, dtype=jnp.int32)

    def per_block(block_index):
        query_block = lax.dynamic_index_in_dim(queries, block_index, 0, keepdims=False)
        query_pos = block_index * TOK_DEV + jnp.arange(TOK_DEV, dtype=jnp.int32)
        allowed = (positions[None, :] <= query_pos[:, None]) & live_all[None, :]

        def per_head(inputs):
            query_head, key_head, value_head = inputs
            scores = jnp.einsum('tgd,sd->gts', query_head.astype(jnp.float32), key_head.astype(jnp.float32)) * score_scale
            scores = jnp.where(allowed[None], scores, -jnp.inf)
            row_peak = lax.optimization_barrier(jnp.max(scores, axis=-1, keepdims=True))
            probs_full = jnp.exp(scores - row_peak)
            row_total = lax.optimization_barrier(jnp.sum(probs_full, axis=-1))
            summed = jnp.einsum('gts,sd->tgd', rounded(probs_full), value_head.astype(jnp.float32))
            return summed / row_total.T[:, :, None]
        heads_out = lax.map(per_head, (query_block.transpose(1, 0, 2, 3), keys_all, values_all))
        return heads_out.transpose(1, 0, 2, 3).reshape(TOK_DEV, QUERY_HEAD_COUNT * HEAD_DIM)
    outputs = lax.map(per_block, jnp.arange(N_SEQ, dtype=jnp.int32))
    outputs = outputs.reshape(TOKEN_SLOTS, QUERY_HEAD_COUNT * HEAD_DIM)
    return jnp.where(live_all[:, None], outputs, 0.0).astype(jnp.bfloat16)

def reference(light_queries, light_keys, light_values, decay_log, norm_gain, soft_queries, soft_keys, soft_values, lengths):
    positions = jnp.arange(TOKEN_SLOTS, dtype=jnp.int32)
    live_all = positions % TOK_DEV < lengths[positions // TOK_DEV]
    light_out = light_reference(light_queries, light_keys, light_values, decay_log, norm_gain, lengths)
    soft_out = soft_reference(soft_queries, soft_keys, soft_values, live_all)
    return (light_out, soft_out)
```

```python
import functools
import math

import jax
import jax.numpy as jnp
from jax import lax
from jax.experimental import pallas as pl
from jax.experimental.pallas import tpu as pltpu
from jax.sharding import PartitionSpec as P

MESH = pl.DeviceIdType.MESH
F32 = jnp.float32
BF16 = jnp.bfloat16
MASKED = -1e30
TICKS = 4


def dot(a, b, contract=(1, 0), precision=None):
    return lax.dot_general(
        a,
        b,
        (((contract[0],), (contract[1],)), ((), ())),
        precision=precision,
        preferred_element_type=F32,
    )


def kernel(
    n,
    up_hops,
    lq_ref,
    lk_ref,
    lv_ref,
    decay_ref,
    gain_ref,
    sq_ref,
    sk_ref,
    sv_ref,
    len_ref,
    lo_ref,
    so_ref,
    kbuf,
    vbuf,
    ebuf,
    obuf,
    state,
    inside,
    qt,
    ot,
    peak,
    total,
    cum,
    cum_t,
    keep,
    bias_ref,
    recv_k,
    recv_v,
    send_k,
    send_v,
    chain_recv,
    chain_send,
):
    down_hops = n - 1 - up_hops
    me = lax.axis_index("seq")
    right, left = lax.rem(me + 1, n), lax.rem(me + n - 1, n)
    toks, width = sk_ref.shape
    heads = decay_ref.shape[1]
    score_scale = width ** (-0.5)
    exp2_scale = score_scale * math.log2(math.e)

    barrier = pltpu.get_barrier_semaphore()
    for neighbour in (left, right):
        pl.semaphore_signal(barrier, inc=1, device_id={"seq": neighbour}, device_id_type=MESH)
    pl.semaphore_wait(barrier, 2)

    def block_copies(k_src, v_src, s, direction, hop):
        target = right if direction == 0 else left
        return (
            pltpu.make_async_remote_copy(
                src_ref=k_src,
                dst_ref=kbuf.at[s],
                send_sem=send_k.at[direction, hop],
                recv_sem=recv_k.at[s],
                device_id={"seq": target},
                device_id_type=MESH,
            ),
            pltpu.make_async_remote_copy(
                src_ref=v_src,
                dst_ref=vbuf.at[s],
                send_sem=send_v.at[direction, hop],
                recv_sem=recv_v.at[s],
                device_id={"seq": target},
                device_id_type=MESH,
            ),
        )

    def chain_copy(h):
        return pltpu.make_async_remote_copy(
            src_ref=obuf.at[h],
            dst_ref=ebuf.at[h],
            send_sem=chain_send.at[h],
            recv_sem=chain_recv.at[h],
            device_id={"seq": right},
            device_id_type=MESH,
        )

    @pl.when(me < n - 1)
    def _():
        for copy in block_copies(sk_ref, sv_ref, me, 0, 0):
            copy.start()

    @pl.when(me < down_hops)
    def _():
        for copy in block_copies(sk_ref, sv_ref, me, 1, 0):
            copy.start()

    own_length = len_ref[me]
    row_of = lax.broadcasted_iota(jnp.int32, (toks, toks), 0)
    col_of = lax.broadcasted_iota(jnp.int32, (toks, toks), 1)
    live_col = lax.broadcasted_iota(jnp.int32, (toks, heads), 0) < own_length
    masked = jnp.where(live_col, decay_ref[...], 0.0)
    running = dot((row_of >= col_of).astype(F32), masked, precision=lax.Precision.HIGHEST)
    cum[...] = running
    cum_t[...] = dot(
        masked, (row_of <= col_of).astype(F32), (0, 0), precision=lax.Precision.HIGHEST
    )
    keep[...] = jnp.broadcast_to(jnp.exp(cum_t[:, toks - 1 : toks]), (heads, width))
    fading = jnp.where(live_col, jnp.exp(running[toks - 1 : toks, :] - running), 0.0)
    for h in range(heads):
        cols = slice(h * width, (h + 1) * width)
        block_keys = (lk_ref[:, cols].astype(F32) * fading[:, h : h + 1]).astype(BF16)
        own_state = dot(block_keys, lv_ref[:, cols], (0, 0))
        state[h] = own_state

        @pl.when(me == 0)
        def _():
            obuf[h] = own_state.astype(BF16)
            ebuf[h] = jnp.zeros((width, width), BF16)
            chain_copy(h).start()

    causal = row_of >= col_of
    for h in range(heads):
        cols = slice(h * width, (h + 1) * width)
        scores = dot(lq_ref[:, cols], lk_ref[:, cols], (1, 1))
        gaps = jnp.where(causal, cum[:, h : h + 1] - cum_t[h : h + 1, :], MASKED)
        weights = (scores * score_scale * jnp.exp(gaps)).astype(BF16)
        inside[:, cols] = dot(weights, lv_ref[:, cols])

    def attend_head(h, scores, v_t, first):
        block_peak = jnp.max(scores, axis=0, keepdims=True)
        if first:
            new_peak = block_peak
        else:
            old_peak = peak[pl.ds(h, 1), :]
            new_peak = jnp.maximum(old_peak, block_peak)
        probs = jnp.exp2((scores - new_peak) * exp2_scale)
        block_total = jnp.sum(probs, axis=0, keepdims=True)
        block_out = dot(v_t, probs.astype(BF16))
        peak[pl.ds(h, 1), :] = new_peak
        if first:
            total[pl.ds(h, 1), :] = block_total
            ot[h] = block_out
        else:
            shrink = jnp.exp2((old_peak - new_peak) * exp2_scale)
            total[pl.ds(h, 1), :] = total[pl.ds(h, 1), :] * shrink + block_total
            ot[h] = ot[h] * shrink + block_out

    seen = (row_of <= col_of) & (row_of < own_length)
    own_v_t = sv_ref[...].T
    for h in range(heads):
        q_t = sq_ref[:, h * width : (h + 1) * width].T
        qt[h] = q_t
        scores = jnp.where(seen, dot(sk_ref[...], q_t), MASKED)
        attend_head(h, scores, own_v_t, True)

    half = heads // 2

    def attend_block(s, first_head):
        dead = lax.broadcasted_iota(jnp.int32, (toks, width), 0) >= len_ref[s]
        bias_ref[...] = jnp.where(dead, MASKED, 0.0)
        k_block = kbuf[s]
        v_t = vbuf[s].T
        for i in range(half):
            h = first_head + i
            bias = bias_ref[...]
            scores = dot(k_block, qt[h]) + jnp.concatenate([bias] * (toks // width), axis=1)
            attend_head(h, scores, v_t, False)

    def finish_light(h, entering):
        cols = pl.ds(pl.multiple_of(h * width, width), width)
        pick = (lax.broadcasted_iota(jnp.int32, (toks, heads), 1) == h).astype(F32)
        grown = jnp.exp(jnp.sum(cum[...] * pick, axis=1, keepdims=True)) * score_scale
        combined = inside[:, cols] + dot(lq_ref[:, cols], entering) * grown
        mean = jnp.mean(combined * combined, axis=1, keepdims=True)
        normed = combined * lax.rsqrt(mean + 1e-6) * gain_ref[:, cols]
        alive = lax.broadcasted_iota(jnp.int32, (toks, width), 0) < own_length
        lo_ref[:, cols] = jnp.where(alive, normed, 0.0).astype(BF16)

    def tick(t, carry):
        hop = t // TICKS + 1
        phase = lax.rem(t, TICKS)
        up_block = me - hop
        down_block = lax.rem(me + hop, n)
        has_up = (hop <= up_hops) & (up_block >= 0)
        has_down = (hop <= down_hops) & (down_block < down_hops)

        @pl.when((phase == 0) & has_up)
        def _():
            s = up_block
            copies = block_copies(kbuf.at[s], vbuf.at[s], s, 0, hop)
            for copy in copies:
                copy.wait_recv()

                @pl.when((hop < up_hops) & (me < n - 1))
                def _():
                    copy.start()

        @pl.when((phase == 0) & has_down)
        def _():
            s = down_block
            copies = block_copies(kbuf.at[s], vbuf.at[s], s, 1, hop)
            for copy in copies:
                copy.wait_recv()

                @pl.when(hop < down_hops)
                def _():
                    copy.start()

        h = t - me * TICKS

        @pl.when((h >= 0) & (h < heads))
        def _():
            @pl.when(me > 0)
            def _():
                chain_copy(h).wait_recv()

            entering = ebuf[h]

            @pl.when((me > 0) & (me < n - 1))
            def _():
                obuf[h] = (entering.astype(F32) * keep[pl.ds(h, 1), :] + state[h]).astype(BF16)
                chain_copy(h).start()

            finish_light(h, entering)

        @pl.when((phase < 2) & has_up)
        def _():
            attend_block(up_block, phase * half)

        @pl.when((phase >= 2) & has_down & (down_block < me))
        def _():
            attend_block(down_block, (phase - 2) * half)

        return carry

    lax.fori_loop(0, max((n - 1) * TICKS + heads, max(up_hops, down_hops) * TICKS), tick, 0)

    alive_q = lax.broadcasted_iota(jnp.int32, (1, toks), 1) < own_length
    for h in range(heads):
        norm = jnp.where(alive_q, 1.0 / total[h : h + 1, :], 0.0)
        so_ref[:, h * width : (h + 1) * width] = (ot[h] * norm).T.astype(BF16)

    def drain(hop, carry):
        up_block = me - hop
        down_block = lax.rem(me + hop, n)

        @pl.when((hop < up_hops) & (up_block >= 0) & (me < n - 1))
        def _():
            for copy in block_copies(kbuf.at[up_block], vbuf.at[up_block], up_block, 0, hop):
                copy.wait_send()

        @pl.when((hop < down_hops) & (down_block < down_hops))
        def _():
            for copy in block_copies(kbuf.at[down_block], vbuf.at[down_block], down_block, 1, hop):
                copy.wait_send()

        return carry

    lax.fori_loop(0, max(up_hops, down_hops), drain, 0)

    @pl.when(me < n - 1)
    def _():
        for h in range(heads):
            chain_copy(h).wait_send()


def body(n, *args):
    toks, columns = args[0].shape
    width = args[6].shape[1]
    heads = columns // width
    up_hops = (n - 1) // 2
    hops = n - 1 - up_hops
    vmem = pl.BlockSpec(memory_space=pltpu.VMEM)
    smem = pl.BlockSpec(memory_space=pltpu.SMEM)
    gain = args[4].reshape(1, columns)
    out = jax.ShapeDtypeStruct((toks, columns), BF16)
    return pl.pallas_call(
        functools.partial(kernel, n, up_hops),
        out_shape=(out, out),
        in_specs=[vmem] * 8 + [smem],
        out_specs=(vmem, vmem),
        scratch_shapes=[
            pltpu.VMEM((n, toks, width), BF16),
            pltpu.VMEM((n, toks, width), BF16),
            pltpu.VMEM((heads, width, width), BF16),
            pltpu.VMEM((heads, width, width), BF16),
            pltpu.VMEM((heads, width, width), F32),
            pltpu.VMEM((toks, columns), F32),
            pltpu.VMEM((heads, width, toks), BF16),
            pltpu.VMEM((heads, width, toks), F32),
            pltpu.VMEM((heads, toks), F32),
            pltpu.VMEM((heads, toks), F32),
            pltpu.VMEM((toks, heads), F32),
            pltpu.VMEM((heads, toks), F32),
            pltpu.VMEM((heads, width), F32),
            pltpu.VMEM((toks, width), F32),
            pltpu.SemaphoreType.DMA((n,)),
            pltpu.SemaphoreType.DMA((n,)),
            pltpu.SemaphoreType.DMA((2, hops + 1)),
            pltpu.SemaphoreType.DMA((2, hops + 1)),
            pltpu.SemaphoreType.DMA((heads,)),
            pltpu.SemaphoreType.DMA((heads,)),
        ],
        compiler_params=pltpu.CompilerParams(
            collective_id=0, has_side_effects=True, vmem_limit_bytes=48 * 1024 * 1024
        ),
    )(*args[:4], gain, *args[5:])


def solution(mesh):
    tokens = P(("groups", "seq"), ("section", "mp"))
    return jax.shard_map(
        functools.partial(body, mesh.shape["seq"]),
        mesh=mesh,
        in_specs=(tokens,) * 4 + (P(("section", "mp")),) + (tokens,) * 3 + (P("groups"),),
        out_specs=(tokens, tokens),
        check_vma=False,
    )
```

```python
import functools
import math

import jax
import jax.numpy as jnp
from jax import lax
from jax.experimental import pallas as pl
from jax.experimental.pallas import tpu as pltpu
from jax.sharding import PartitionSpec as P

MESH = pl.DeviceIdType.MESH
F32 = jnp.float32
BF16 = jnp.bfloat16
MASKED = -1e30
HOP_TICKS = 5
FIRST_TICK = 0
WRAP_STEP = 3
UP_EXTRA = 1


def dot(a, b, contract=(1, 0), precision=None):
    return lax.dot_general(
        a,
        b,
        (((contract[0],), (contract[1],)), ((), ())),
        precision=precision,
        preferred_element_type=F32,
    )


def kernel(
    n,
    up_hops,
    lq_hbm,
    lk_hbm,
    lv_hbm,
    decay_ref,
    gain_ref,
    sq_hbm,
    sk_hbm,
    sv_hbm,
    len_ref,
    lo_ref,
    so_ref,
    lq_ref,
    lk_ref,
    lv_ref,
    sq_ref,
    kbuf,
    vbuf,
    ebuf,
    obuf,
    state,
    inside,
    qt,
    ot,
    peak,
    total,
    cum,
    cum_t,
    keep,
    bias_ref,
    vt_ref,
    ready_sem,
    load_sem,
    recv_k,
    recv_v,
    send_k,
    send_v,
    chain_recv,
    chain_send,
):
    down_hops = n - 1 - up_hops
    me = lax.axis_index("seq")
    last = n - 1
    right = jnp.minimum(me + 1, last)
    left = jnp.where(me == 0, last, me - 1)
    toks, width = sk_hbm.shape
    heads = decay_ref.shape[0]
    score_scale = width ** (-0.5)
    exp2_scale = score_scale * math.log2(math.e)

    loads = {}
    for i, (name, src, dst) in enumerate(
        (
            ("sk", sk_hbm, kbuf.at[me]),
            ("sv", sv_hbm, vbuf.at[me]),
            ("lk", lk_hbm, lk_ref),
            ("lv", lv_hbm, lv_ref),
            ("lq", lq_hbm, lq_ref),
            ("sq", sq_hbm, sq_ref),
        )
    ):
        loads[name] = pltpu.make_async_copy(src, dst, load_sem.at[i])
        loads[name].start()

    barrier = pltpu.get_barrier_semaphore()

    def tell(semaphore, device):
        pl.semaphore_signal(semaphore, inc=1, device_id={"seq": device}, device_id_type=MESH)

    @pl.when(me > 0)
    def _():
        tell(barrier, me - 1)

    @pl.when(me < last)
    def _():
        tell(barrier, me + 1)

    @pl.when(me == 0)
    def _():
        tell(barrier, last)

    @pl.when(me == 0)
    def _():
        pl.semaphore_wait(barrier, 1)

    @pl.when(me > 0)
    def _():
        pl.semaphore_wait(barrier, 2)

    @pl.when(me == last)
    def _():
        tell(ready_sem, 0)

    def block_copies(s, direction):
        target = right if direction == 0 else left
        return (
            pltpu.make_async_remote_copy(
                src_ref=kbuf.at[s],
                dst_ref=kbuf.at[s],
                send_sem=send_k.at[direction, s],
                recv_sem=recv_k.at[s],
                device_id={"seq": target},
                device_id_type=MESH,
            ),
            pltpu.make_async_remote_copy(
                src_ref=vbuf.at[s],
                dst_ref=vbuf.at[s],
                send_sem=send_v.at[direction, s],
                recv_sem=recv_v.at[s],
                device_id={"seq": target},
                device_id_type=MESH,
            ),
        )

    def chain_copy(h):
        return pltpu.make_async_remote_copy(
            src_ref=obuf.at[h],
            dst_ref=ebuf.at[h],
            send_sem=chain_send.at[h],
            recv_sem=chain_recv.at[h],
            device_id={"seq": right},
            device_id_type=MESH,
        )

    loads["sk"].wait()
    loads["sv"].wait()

    @pl.when(me < last)
    def _():
        for copy in block_copies(me, 0):
            copy.start()

    @pl.when((me > 0) & (me < down_hops))
    def _():
        for copy in block_copies(me, 1):
            copy.start()

    own_length = len_ref[me]
    row_of = lax.broadcasted_iota(jnp.int32, (toks, toks), 0)
    col_of = lax.broadcasted_iota(jnp.int32, (toks, toks), 1)
    until = (row_of <= col_of).astype(F32).astype(BF16)
    live_row = lax.broadcasted_iota(jnp.int32, (heads, toks), 1) < own_length
    masked = jnp.where(live_row, decay_ref[...], 0.0)
    high = masked.astype(BF16).astype(F32)
    middle = (masked - high).astype(BF16).astype(F32)
    low = masked - high - middle
    sums = dot(jnp.concatenate([high, middle, low], axis=0).astype(BF16), until)
    running_t = sums[:heads] + sums[heads : 2 * heads] + sums[2 * heads :]
    cum_t[...] = running_t
    keep[...] = jnp.broadcast_to(jnp.exp(running_t[:, toks - 1 :]), (heads, width))
    cum[...] = running_t.T
    faded_t = jnp.where(live_row, jnp.exp(running_t[:, toks - 1 :] - running_t), 0.0)
    fading = faded_t.T

    loads["lk"].wait()
    loads["lv"].wait()
    for h in range(heads):
        cols = slice(h * width, (h + 1) * width)
        block_keys = (lk_ref[:, cols].astype(F32) * fading[:, h : h + 1]).astype(BF16)
        state[h] = dot(block_keys, lv_ref[:, cols], (0, 0))

    @pl.when(me == 0)
    def _():
        for h in range(heads):
            obuf[h] = state[h].astype(BF16)
            ebuf[h] = jnp.zeros((width, width), BF16)
        for h in range(heads):
            chain_copy(h).start()

    loads["lq"].wait()
    causal = row_of >= col_of

    def light_scores(h):
        cols = slice(h * width, (h + 1) * width)
        return dot(lq_ref[:, cols], lk_ref[:, cols], (1, 1))

    ahead = [light_scores(0), light_scores(1)]
    for h in range(heads):
        cols = slice(h * width, (h + 1) * width)
        gaps = jnp.where(causal, cum[:, h : h + 1] - cum_t[h : h + 1, :], MASKED)
        weights = (ahead[h] * score_scale * jnp.exp(gaps)).astype(BF16)
        if h + 2 < heads:
            ahead.append(light_scores(h + 2))
        inside[:, cols] = dot(weights, lv_ref[:, cols])

    def attend(hs, scores_of, values_t, first):
        ahead = [scores_of(h) for h in hs[:2]]
        for i, h in enumerate(hs):
            scores = ahead[i]
            row = slice(h, h + 1)
            new_peak = jnp.max(scores, axis=0, keepdims=True)
            if not first:
                old_peak = peak[row, :]
                new_peak = jnp.maximum(old_peak, new_peak)
            probs = jnp.exp2((scores - new_peak) * exp2_scale)
            block_total = jnp.sum(probs, axis=0, keepdims=True)
            if i + 2 < len(hs):
                ahead.append(scores_of(hs[i + 2]))
            block_out = dot(values_t, probs.astype(BF16))
            peak[row, :] = new_peak
            if first:
                total[row, :] = block_total
                ot[h] = block_out
            else:
                shrink = jnp.exp2((old_peak - new_peak) * exp2_scale)
                total[row, :] = total[row, :] * shrink + block_total
                ot[h] = ot[h] * shrink + block_out

    loads["sq"].wait()
    seen = (row_of <= col_of) & (row_of < own_length)
    own_keys = kbuf[me]
    for h in range(heads):
        qt[h] = sq_ref[:, h * width : (h + 1) * width].T
    attend(
        tuple(range(heads)),
        lambda h: jnp.where(seen, dot(own_keys, qt[h]), MASKED),
        vbuf[me].T,
        True,
    )

    halves = (tuple(range(heads // 2)), tuple(range(heads // 2, heads)))
    per_tick = 2
    events = heads // per_tick

    def finish_light(h, entering):
        cols = slice(h * width, (h + 1) * width)
        grown = jnp.exp(cum[:, h : h + 1]) * score_scale
        combined = inside[:, cols] + dot(lq_ref[:, cols], entering) * grown
        mean = jnp.mean(combined * combined, axis=1, keepdims=True)
        normed = combined * lax.rsqrt(mean + 1e-6) * gain_ref[:, cols]
        alive = lax.broadcasted_iota(jnp.int32, (toks, width), 0) < own_length
        lo_ref[:, cols] = jnp.where(alive, normed, 0.0).astype(BF16)

    def first_tick(device):
        return (device * HOP_TICKS) // 4 + FIRST_TICK

    def chain_events(t):
        for j in range(events):

            @pl.when(t - first_tick(me) == j)
            def _():
                hs = range(j * per_tick, (j + 1) * per_tick)
                for h in hs:

                    @pl.when(me > 0)
                    def _():
                        chain_copy(h).wait_recv()

                    @pl.when((me > 0) & (me < last))
                    def _():
                        obuf[h] = (ebuf[h].astype(F32) * keep[h : h + 1, :] + state[h]).astype(BF16)
                        chain_copy(h).start()

                for h in hs:
                    finish_light(h, ebuf[h])

    def finish_soft():
        alive_q = lax.broadcasted_iota(jnp.int32, (1, toks), 1) < own_length
        for h in range(heads):
            norm = jnp.where(alive_q, 1.0 / total[h : h + 1, :], 0.0)
            so_ref[:, h * width : (h + 1) * width] = (ot[h] * norm).astype(BF16).T

    def plan(hop):
        up_block = me - hop
        has_up = (hop >= 1) & (hop <= up_hops) & (up_block >= 0)
        before = me < down_hops
        down_hop = hop - jnp.where(me == 0, WRAP_STEP, 0)
        down_block = jnp.where(before, me + down_hop, me + down_hop - n)
        arrives = before | (down_hop <= down_hops)
        has_down = (down_hop > 0) & arrives & (down_block >= 0) & (down_block < down_hops)
        return up_block, has_up, before, down_hop, down_block, has_down, has_down & (me >= down_hops)

    def pass_on(hop, part):
        up_block, has_up, before, down_hop, down_block, has_down, _ = plan(hop)

        @pl.when(has_up)
        def _():
            copy = block_copies(up_block, 0)[part]
            copy.wait_recv()

            @pl.when((hop < up_hops) & (me < last))
            def _():
                copy.start()

        @pl.when(has_down)
        def _():
            copy = block_copies(down_block, 1)[part]
            copy.wait_recv()

            @pl.when(before | (down_hop < down_hops))
            def _():
                copy.start()

    def attend_half(hop, half):
        up_block, has_up, _, _, down_block, _, use_down = plan(hop)

        @pl.when(has_up | use_down)
        def _():
            blocks = (jnp.where(has_up, up_block, me), jnp.where(use_down, down_block, me))
            if half == 0:
                used = (has_up, use_down)
                rows = lax.broadcasted_iota(jnp.int32, (toks, width), 0)
                for i in range(2):
                    length = jnp.where(used[i], len_ref[blocks[i]], 0)
                    span = slice(i * toks, (i + 1) * toks)
                    bias_ref[span, :] = jnp.where(rows < length, 0.0, MASKED)
                    vt_ref[:, span] = vbuf[blocks[i]].T
            keys = jnp.concatenate([kbuf[s] for s in blocks], axis=0)

            def scores_of(h):
                bias = bias_ref[...]
                return dot(keys, qt[h]) + jnp.concatenate([bias] * (toks // width), axis=1)

            attend(halves[half], scores_of, vt_ref[...], False)

    def step(hop, carry):
        @pl.when((me == 0) & (hop == WRAP_STEP))
        def _():
            pl.semaphore_wait(ready_sem, 1)
            for copy in block_copies(me, 1):
                copy.start()

        pass_on(hop, 0)
        chain_events(2 * hop - 2)
        attend_half(hop - 1, 1)
        pass_on(hop, 1)

        @pl.when(hop == max(up_hops, down_hops) + 1)
        def _():
            finish_soft()

        chain_events(2 * hop - 1)
        attend_half(hop, 0)
        return carry

    steps = max(
        up_hops + 1,
        down_hops + 1 + WRAP_STEP,
        (first_tick(last) + events + 1) // 2,
    )
    lax.fori_loop(1, steps + 1, step, 0)

    def drain(s, carry):
        @pl.when((s <= me) & (me - s < up_hops) & (me < last))
        def _():
            for copy in block_copies(s, 0):
                copy.wait_send()

        passed = me <= s
        wrapped = me > s + up_hops + 1

        @pl.when((s < down_hops) & (passed | wrapped))
        def _():
            for copy in block_copies(s, 1):
                copy.wait_send()

        return carry

    lax.fori_loop(0, n, drain, 0)

    @pl.when(me < last)
    def _():
        for h in range(heads):
            chain_copy(h).wait_send()


def body(n, *args):
    toks, columns = args[0].shape
    width = args[6].shape[1]
    heads = columns // width
    up_hops = n // 2 + UP_EXTRA
    vmem = pl.BlockSpec(memory_space=pltpu.VMEM)
    hbm = pl.BlockSpec(memory_space=pltpu.HBM)
    smem = pl.BlockSpec(memory_space=pltpu.SMEM)
    gain = args[4].reshape(1, columns)
    out = jax.ShapeDtypeStruct((toks, columns), BF16)
    return pl.pallas_call(
        functools.partial(kernel, n, up_hops),
        out_shape=(out, out),
        in_specs=[hbm] * 3 + [vmem] * 2 + [hbm] * 3 + [smem],
        out_specs=(vmem, vmem),
        scratch_shapes=[
            pltpu.VMEM((toks, columns), BF16),
            pltpu.VMEM((toks, columns), BF16),
            pltpu.VMEM((toks, columns), BF16),
            pltpu.VMEM((toks, columns), BF16),
            pltpu.VMEM((n, toks, width), BF16),
            pltpu.VMEM((n, toks, width), BF16),
            pltpu.VMEM((heads, width, width), BF16),
            pltpu.VMEM((heads, width, width), BF16),
            pltpu.VMEM((heads, width, width), F32),
            pltpu.VMEM((toks, columns), F32),
            pltpu.VMEM((heads, width, toks), BF16),
            pltpu.VMEM((heads, width, toks), F32),
            pltpu.VMEM((heads, toks), F32),
            pltpu.VMEM((heads, toks), F32),
            pltpu.VMEM((toks, heads), F32),
            pltpu.VMEM((heads, toks), F32),
            pltpu.VMEM((heads, width), F32),
            pltpu.VMEM((2 * toks, width), F32),
            pltpu.VMEM((width, 2 * toks), BF16),
            pltpu.SemaphoreType.REGULAR,
            pltpu.SemaphoreType.DMA((6,)),
            pltpu.SemaphoreType.DMA((n,)),
            pltpu.SemaphoreType.DMA((n,)),
            pltpu.SemaphoreType.DMA((2, n)),
            pltpu.SemaphoreType.DMA((2, n)),
            pltpu.SemaphoreType.DMA((heads,)),
            pltpu.SemaphoreType.DMA((heads,)),
        ],
        compiler_params=pltpu.CompilerParams(
            collective_id=0, has_side_effects=True, vmem_limit_bytes=67_043_328
        ),
    )(*args[:3], args[3].T, gain, *args[5:])


def solution(mesh):
    tokens = P(("groups", "seq"), ("section", "mp"))
    return jax.shard_map(
        functools.partial(body, mesh.shape["seq"]),
        mesh=mesh,
        in_specs=(tokens,) * 4 + (P(("section", "mp")),) + (tokens,) * 3 + (P("groups"),),
        out_specs=(tokens, tokens),
        check_vma=False,
    )
```

```python
import functools
import math

import jax
import jax.numpy as jnp
from jax import lax
from jax.experimental import pallas as pl
from jax.experimental.pallas import tpu as pltpu
from jax.sharding import PartitionSpec as P

MESH = pl.DeviceIdType.MESH
F32 = jnp.float32
BF16 = jnp.bfloat16
MASKED = -1e30
HOP_TICKS = 5
FIRST_TICK = 0
WRAP_STEP = 3
UP_EXTRA = 1


def dot(a, b, contract=(1, 0), precision=None):
    return lax.dot_general(
        a,
        b,
        (((contract[0],), (contract[1],)), ((), ())),
        precision=precision,
        preferred_element_type=F32,
    )


def kernel(
    n,
    up_hops,
    lq_hbm,
    lk_hbm,
    lv_hbm,
    decay_ref,
    gain_ref,
    sq_hbm,
    sk_hbm,
    sv_hbm,
    len_ref,
    lo_ref,
    so_ref,
    lq_ref,
    lk_ref,
    lv_ref,
    sq_ref,
    kbuf,
    vbuf,
    ebuf,
    obuf,
    state,
    inside,
    qt,
    ot,
    peak,
    total,
    cum,
    cum_t,
    keep,
    bias_ref,
    vt_ref,
    ready_sem,
    load_sem,
    recv_k,
    recv_v,
    send_k,
    send_v,
    chain_recv,
    chain_send,
):
    down_hops = n - 1 - up_hops
    me = lax.axis_index("seq")
    last = n - 1
    right = jnp.minimum(me + 1, last)
    left = jnp.where(me == 0, last, me - 1)
    toks, width = sk_hbm.shape
    heads = decay_ref.shape[0]
    score_scale = width ** (-0.5)
    exp2_scale = score_scale * math.log2(math.e)

    loads = {}
    for i, (name, src, dst) in enumerate(
        (
            ("sk", sk_hbm, kbuf.at[me]),
            ("sv", sv_hbm, vbuf.at[me]),
            ("lk", lk_hbm, lk_ref),
            ("lv", lv_hbm, lv_ref),
            ("lq", lq_hbm, lq_ref),
            ("sq", sq_hbm, sq_ref),
        )
    ):
        loads[name] = pltpu.make_async_copy(src, dst, load_sem.at[i])
        loads[name].start()

    barrier = pltpu.get_barrier_semaphore()

    def tell(semaphore, device):
        pl.semaphore_signal(semaphore, inc=1, device_id={"seq": device}, device_id_type=MESH)

    @pl.when(me > 0)
    def _():
        tell(barrier, me - 1)

    @pl.when(me < last)
    def _():
        tell(barrier, me + 1)

    @pl.when(me == 0)
    def _():
        tell(barrier, last)

    @pl.when(me == 0)
    def _():
        pl.semaphore_wait(barrier, 1)

    @pl.when(me > 0)
    def _():
        pl.semaphore_wait(barrier, 2)

    @pl.when(me == last)
    def _():
        tell(ready_sem, 0)

    def block_copies(s, direction):
        target = right if direction == 0 else left
        return (
            pltpu.make_async_remote_copy(
                src_ref=kbuf.at[s],
                dst_ref=kbuf.at[s],
                send_sem=send_k.at[direction, s],
                recv_sem=recv_k.at[s],
                device_id={"seq": target},
                device_id_type=MESH,
            ),
            pltpu.make_async_remote_copy(
                src_ref=vbuf.at[s],
                dst_ref=vbuf.at[s],
                send_sem=send_v.at[direction, s],
                recv_sem=recv_v.at[s],
                device_id={"seq": target},
                device_id_type=MESH,
            ),
        )

    def chain_copy(h):
        return pltpu.make_async_remote_copy(
            src_ref=obuf.at[h],
            dst_ref=ebuf.at[h],
            send_sem=chain_send.at[h],
            recv_sem=chain_recv.at[h],
            device_id={"seq": right},
            device_id_type=MESH,
        )

    loads["sk"].wait()
    loads["sv"].wait()

    @pl.when(me < last)
    def _():
        for copy in block_copies(me, 0):
            copy.start()

    @pl.when((me > 0) & (me < down_hops))
    def _():
        for copy in block_copies(me, 1):
            copy.start()

    own_length = len_ref[me]
    row_of = lax.broadcasted_iota(jnp.int32, (toks, toks), 0)
    col_of = lax.broadcasted_iota(jnp.int32, (toks, toks), 1)
    until = (row_of <= col_of).astype(F32).astype(BF16)
    live_row = lax.broadcasted_iota(jnp.int32, (heads, toks), 1) < own_length
    masked = jnp.where(live_row, decay_ref[...], 0.0)
    high = masked.astype(BF16).astype(F32)
    middle = (masked - high).astype(BF16).astype(F32)
    low = masked - high - middle
    sums = dot(jnp.concatenate([high, middle, low], axis=0).astype(BF16), until)
    running_t = sums[:heads] + sums[heads : 2 * heads] + sums[2 * heads :]
    cum_t[...] = running_t
    keep[...] = jnp.broadcast_to(jnp.exp(running_t[:, toks - 1 :]), (heads, width))
    cum[...] = running_t.T
    faded_t = jnp.where(live_row, jnp.exp(running_t[:, toks - 1 :] - running_t), 0.0)
    fading = faded_t.T

    loads["lk"].wait()
    loads["lv"].wait()
    for h in range(heads):
        cols = slice(h * width, (h + 1) * width)
        block_keys = (lk_ref[:, cols].astype(F32) * fading[:, h : h + 1]).astype(BF16)
        state[h] = dot(block_keys, lv_ref[:, cols], (0, 0))

    @pl.when(me == 0)
    def _():
        for h in range(heads):
            obuf[h] = state[h].astype(BF16)
            ebuf[h] = jnp.zeros((width, width), BF16)
        for h in range(heads):
            chain_copy(h).start()

    loads["lq"].wait()
    causal = row_of >= col_of

    def light_scores(h):
        cols = slice(h * width, (h + 1) * width)
        return dot(lq_ref[:, cols], lk_ref[:, cols], (1, 1))

    ahead = [light_scores(0), light_scores(1)]
    for h in range(heads):
        cols = slice(h * width, (h + 1) * width)
        gaps = jnp.where(causal, cum[:, h : h + 1] - cum_t[h : h + 1, :], MASKED)
        weights = (ahead[h] * score_scale * jnp.exp(gaps)).astype(BF16)
        if h + 2 < heads:
            ahead.append(light_scores(h + 2))
        inside[:, cols] = dot(weights, lv_ref[:, cols])

    def attend(hs, scores_of, values_t, first):
        ahead = [scores_of(h) for h in hs[:2]]
        for i, h in enumerate(hs):
            scores = ahead[i]
            row = slice(h, h + 1)
            new_peak = jnp.max(scores, axis=0, keepdims=True)
            if not first:
                old_peak = peak[row, :]
                new_peak = jnp.maximum(old_peak, new_peak)
            probs = jnp.exp2((scores - new_peak) * exp2_scale)
            block_total = jnp.sum(probs, axis=0, keepdims=True)
            if i + 2 < len(hs):
                ahead.append(scores_of(hs[i + 2]))
            block_out = dot(values_t, probs.astype(BF16))
            peak[row, :] = new_peak
            if first:
                total[row, :] = block_total
                ot[h] = block_out
            else:
                shrink = jnp.exp2((old_peak - new_peak) * exp2_scale)
                total[row, :] = total[row, :] * shrink + block_total
                ot[h] = ot[h] * shrink + block_out

    loads["sq"].wait()
    seen = (row_of <= col_of) & (row_of < own_length)
    own_keys = kbuf[me]
    for h in range(heads):
        qt[h] = sq_ref[:, h * width : (h + 1) * width].T
    attend(
        tuple(range(heads)),
        lambda h: jnp.where(seen, dot(own_keys, qt[h]), MASKED),
        vbuf[me].T,
        True,
    )

    halves = (tuple(range(heads // 2)), tuple(range(heads // 2, heads)))
    per_tick = 4
    events = heads // per_tick

    def finish_light(h, entering):
        cols = slice(h * width, (h + 1) * width)
        grown = jnp.exp(cum[:, h : h + 1]) * score_scale
        combined = inside[:, cols] + dot(lq_ref[:, cols], entering) * grown
        mean = jnp.mean(combined * combined, axis=1, keepdims=True)
        normed = combined * lax.rsqrt(mean + 1e-6) * gain_ref[:, cols]
        alive = lax.broadcasted_iota(jnp.int32, (toks, width), 0) < own_length
        lo_ref[:, cols] = jnp.where(alive, normed, 0.0).astype(BF16)

    def first_tick(device):
        return (device * HOP_TICKS) // 4 + FIRST_TICK

    def chain_events(t):
        for j in range(events):

            @pl.when(t - first_tick(me) == j)
            def _():
                hs = range(j * per_tick, (j + 1) * per_tick)
                for h in hs:

                    @pl.when(me > 0)
                    def _():
                        chain_copy(h).wait_recv()

                    @pl.when((me > 0) & (me < last))
                    def _():
                        obuf[h] = (ebuf[h].astype(F32) * keep[h : h + 1, :] + state[h]).astype(BF16)
                        chain_copy(h).start()

                for h in hs:
                    finish_light(h, ebuf[h])

    def finish_soft():
        alive_q = lax.broadcasted_iota(jnp.int32, (1, toks), 1) < own_length
        for h in range(heads):
            norm = jnp.where(alive_q, 1.0 / total[h : h + 1, :], 0.0)
            so_ref[:, h * width : (h + 1) * width] = (ot[h] * norm).astype(BF16).T

    def plan(hop):
        up_block = me - hop
        has_up = (hop >= 1) & (hop <= up_hops) & (up_block >= 0)
        before = me < down_hops
        down_hop = hop - jnp.where(me == 0, WRAP_STEP, 0)
        down_block = jnp.where(before, me + down_hop, me + down_hop - n)
        arrives = before | (down_hop <= down_hops)
        has_down = (down_hop > 0) & arrives & (down_block >= 0) & (down_block < down_hops)
        return up_block, has_up, before, down_hop, down_block, has_down, has_down & (me >= down_hops)

    def pass_on(hop, part):
        up_block, has_up, before, down_hop, down_block, has_down, _ = plan(hop)

        @pl.when(has_up)
        def _():
            copy = block_copies(up_block, 0)[part]
            copy.wait_recv()

            @pl.when((hop < up_hops) & (me < last))
            def _():
                copy.start()

        @pl.when(has_down)
        def _():
            copy = block_copies(down_block, 1)[part]
            copy.wait_recv()

            @pl.when(before | (down_hop < down_hops))
            def _():
                copy.start()

    def attend_half(hop, half):
        up_block, has_up, _, _, down_block, _, use_down = plan(hop)

        @pl.when(has_up | use_down)
        def _():
            blocks = (jnp.where(has_up, up_block, me), jnp.where(use_down, down_block, me))
            if half == 0:
                used = (has_up, use_down)
                rows = lax.broadcasted_iota(jnp.int32, (toks, width), 0)
                for i in range(2):
                    length = jnp.where(used[i], len_ref[blocks[i]], 0)
                    span = slice(i * toks, (i + 1) * toks)
                    bias_ref[span, :] = jnp.where(rows < length, 0.0, MASKED)
                    vt_ref[:, span] = vbuf[blocks[i]].T
            keys = jnp.concatenate([kbuf[s] for s in blocks], axis=0)

            def scores_of(h):
                bias = bias_ref[...]
                return dot(keys, qt[h]) + jnp.concatenate([bias] * (toks // width), axis=1)

            attend(halves[half], scores_of, vt_ref[...], False)

    def step(hop, carry):
        @pl.when((me == 0) & (hop == WRAP_STEP))
        def _():
            pl.semaphore_wait(ready_sem, 1)
            for copy in block_copies(me, 1):
                copy.start()

        pass_on(hop, 0)
        chain_events(2 * hop - 2)
        attend_half(hop - 1, 1)
        pass_on(hop, 1)

        @pl.when(hop == max(up_hops, down_hops) + 1)
        def _():
            finish_soft()

        chain_events(2 * hop - 1)
        attend_half(hop, 0)
        return carry

    steps = max(
        up_hops + 1,
        down_hops + 1 + WRAP_STEP,
        (first_tick(last) + events + 1) // 2,
    )
    lax.fori_loop(1, steps + 1, step, 0)

    def drain(s, carry):
        @pl.when((s <= me) & (me - s < up_hops) & (me < last))
        def _():
            for copy in block_copies(s, 0):
                copy.wait_send()

        passed = me <= s
        wrapped = me > s + up_hops + 1

        @pl.when((s < down_hops) & (passed | wrapped))
        def _():
            for copy in block_copies(s, 1):
                copy.wait_send()

        return carry

    lax.fori_loop(0, n, drain, 0)

    @pl.when(me < last)
    def _():
        for h in range(heads):
            chain_copy(h).wait_send()


def body(n, *args):
    toks, columns = args[0].shape
    width = args[6].shape[1]
    heads = columns // width
    up_hops = n // 2 + UP_EXTRA
    vmem = pl.BlockSpec(memory_space=pltpu.VMEM)
    hbm = pl.BlockSpec(memory_space=pltpu.HBM)
    smem = pl.BlockSpec(memory_space=pltpu.SMEM)
    gain = args[4].reshape(1, columns)
    out = jax.ShapeDtypeStruct((toks, columns), BF16)
    return pl.pallas_call(
        functools.partial(kernel, n, up_hops),
        out_shape=(out, out),
        in_specs=[hbm] * 3 + [vmem] * 2 + [hbm] * 3 + [smem],
        out_specs=(vmem, vmem),
        scratch_shapes=[
            pltpu.VMEM((toks, columns), BF16),
            pltpu.VMEM((toks, columns), BF16),
            pltpu.VMEM((toks, columns), BF16),
            pltpu.VMEM((toks, columns), BF16),
            pltpu.VMEM((n, toks, width), BF16),
            pltpu.VMEM((n, toks, width), BF16),
            pltpu.VMEM((heads, width, width), BF16),
            pltpu.VMEM((heads, width, width), BF16),
            pltpu.VMEM((heads, width, width), F32),
            pltpu.VMEM((toks, columns), F32),
            pltpu.VMEM((heads, width, toks), BF16),
            pltpu.VMEM((heads, width, toks), F32),
            pltpu.VMEM((heads, toks), F32),
            pltpu.VMEM((heads, toks), F32),
            pltpu.VMEM((toks, heads), F32),
            pltpu.VMEM((heads, toks), F32),
            pltpu.VMEM((heads, width), F32),
            pltpu.VMEM((2 * toks, width), F32),
            pltpu.VMEM((width, 2 * toks), BF16),
            pltpu.SemaphoreType.REGULAR,
            pltpu.SemaphoreType.DMA((6,)),
            pltpu.SemaphoreType.DMA((n,)),
            pltpu.SemaphoreType.DMA((n,)),
            pltpu.SemaphoreType.DMA((2, n)),
            pltpu.SemaphoreType.DMA((2, n)),
            pltpu.SemaphoreType.DMA((heads,)),
            pltpu.SemaphoreType.DMA((heads,)),
        ],
        compiler_params=pltpu.CompilerParams(
            collective_id=0, has_side_effects=True, vmem_limit_bytes=67_043_328
        ),
    )(*args[:3], args[3].T, gain, *args[5:])


def solution(mesh):
    tokens = P(("groups", "seq"), ("section", "mp"))
    return jax.shard_map(
        functools.partial(body, mesh.shape["seq"]),
        mesh=mesh,
        in_specs=(tokens,) * 4 + (P(("section", "mp")),) + (tokens,) * 3 + (P("groups"),),
        out_specs=(tokens, tokens),
        check_vma=False,
    )
```
